32 devices in a mesh: section: 2 (over x), expert: 16 (over z, y, core).
Axes of the slice: x: 2, y: 2, z: 4, core: 2. Of those that a mesh axis runs over, the one named last changes fastest.
Arguments:
- images: bfloat16 [32, 256, 1408], P(('section', 'expert')), may hold values from -6 to 6
- norm_gain: bfloat16 [1408], replicated, may hold values from 0.5 to 1.5
- slot_map: bfloat16 [1408, 16], replicated, may hold values from -0.15625 to 0.15625
- logit_scale: float32 [1], replicated, may hold values from 30 to 80
- up_weight: bfloat16 [16, 5120, 1408], P('expert', 'section'), may hold values from -0.625 to 0.625
- down_weight: bfloat16 [16, 5120, 1408], P('expert', 'section'), may hold values from -0.3125 to 0.3125
Outputs:
- block_out: bfloat16 [32, 256, 1408], P(('section', 'expert'))
The draws below stay inside these ranges and needn't reach their ends.
All inputs are finite; a program needn't handle non-finite values.
Results may differ from the reference program's by a relative error of at most 0.011.
Values may be sent and summed in bfloat16 or wider, within the bound.
A program may use at most 64 MiB of HBM per device.

```python
import math
import jax
import jax.numpy as jnp
from jax import lax

D = 1408
FF = 5120
TOK = 256
EXPERTS = 16
IMAGES = 32


def levels(rng, extent, shards, low, top_value):
    def one(axis_at, shards_of):
        heights = jax.random.uniform(jax.random.fold_in(jax.random.fold_in(rng, 6), axis_at), (shards_of,), jnp.float32, low / len(shards), top_value / len(shards))
        return jnp.repeat(jnp.exp(heights), extent[axis_at] // shards_of).reshape((-1,) + (1,) * (len(extent) - axis_at - 1))

    loudness = one(*shards[0])
    for cut in shards[1:]:
        loudness = loudness * one(*cut)
    return loudness


def centred(own_key, extent, deviation, reach, split=(), kind=jnp.bfloat16):
    level = levels(own_key, extent, split, -0.22, 0.18) if split else 1.0
    result = jax.random.normal(own_key, extent, jnp.float32) * deviation * level
    return jnp.minimum(jnp.maximum(result, -reach), reach).astype(kind)


def setup_inputs(seed: int = 0) -> dict:
    key_list = jax.random.split(jax.random.key(seed), 7)
    images = centred(key_list[0], (IMAGES, TOK, D), 1.0, 6.0, ((0, 32),))
    norm_gain = jnp.clip(1.0 + 0.1 * jax.random.normal(key_list[1], (D,), jnp.float32), 0.5, 1.5).astype(jnp.bfloat16)
    slot_map = centred(key_list[2], (D, EXPERTS), D ** -0.5, 0.15625)
    logit_scale = jnp.clip(jnp.exp(jax.random.uniform(key_list[3], (1,), jnp.float32, math.log(30.0), math.log(80.0))), 30.0, 80.0)
    up_weight = centred(key_list[4], (EXPERTS, FF, D), (4.0 / D ** 0.5), 0.625, ((0, 16), (1, 2)))
    down_weight = centred(key_list[5], (EXPERTS, FF, D), (4.0 / FF ** 0.5), 0.3125, ((0, 16), (1, 2)))
    return dict(images=images, norm_gain=norm_gain, slot_map=slot_map, logit_scale=logit_scale, up_weight=up_weight, down_weight=down_weight)


epsilon = 1e-06

def normalize(inputs, gain_row):
    values = inputs.astype(jnp.float32)
    spread = lax.optimization_barrier(jnp.mean(values * values, axis=-1, keepdims=True))
    return (values * lax.rsqrt(spread + epsilon) * gain_row.astype(jnp.float32)).astype(jnp.bfloat16)

def weights_from(raw, normed, slot_cols, scale_now):
    values = normed.astype(jnp.float32)
    token_norm = jnp.sqrt(lax.optimization_barrier(jnp.sum(values * values, axis=-1)) + epsilon)
    columns = slot_cols.astype(jnp.float32)
    column_norm = jnp.sqrt(lax.optimization_barrier(jnp.sum(columns * columns, axis=0)) + epsilon)
    logits = scale_now * raw / (token_norm[:, None, :] * column_norm[None, :, None])
    scores = jnp.exp(logits)
    dispatch = (scores / lax.optimization_barrier(jnp.sum(scores, axis=-1, keepdims=True))).astype(jnp.bfloat16)
    combine = (scores / lax.optimization_barrier(jnp.sum(scores, axis=1, keepdims=True))).astype(jnp.bfloat16)
    return (dispatch, combine)

def reference(images, norm_gain, slot_map, logit_scale, up_weight, down_weight):
    normed = normalize(images, norm_gain)
    raw = jnp.einsum('itd,de->iet', normed.astype(jnp.float32), slot_map.astype(jnp.float32))
    dispatch, combine = weights_from(raw, normed, slot_map, logit_scale[0])
    slot_in = jnp.einsum('iet,itd->eid', dispatch.astype(jnp.float32), normed.astype(jnp.float32)).astype(jnp.bfloat16)
    hidden = jax.nn.gelu(jnp.einsum('eid,efd->eif', slot_in.astype(jnp.float32), up_weight.astype(jnp.float32))).astype(jnp.bfloat16)
    slot_out = jnp.einsum('eif,efd->eid', hidden.astype(jnp.float32), down_weight.astype(jnp.float32)).astype(jnp.bfloat16)
    mixed = jnp.einsum('iet,eid->itd', combine.astype(jnp.float32), slot_out.astype(jnp.float32))
    return (images.astype(jnp.float32) + mixed).astype(jnp.bfloat16)
```

```python
import functools

import jax
import jax.numpy as jnp
from jax import lax
from jax.experimental import pallas as pl
from jax.experimental.pallas import tpu as pltpu
from jax.sharding import PartitionSpec as P

epsilon = 1e-06
MESH = pl.DeviceIdType.MESH
NT = (((1,), (1,)), ((), ()))
TN = (((0,), (0,)), ((), ()))


def split_of(total, most, unit):
    best = unit
    for size in range(unit, most + 1, unit):
        if total % size == 0:
            best = size
    return best


def kernel(
    sections, experts, chunk,
    x_hbm, gain_ref, slot_ref, scale_ref, up_hbm, down_hbm,
    out_hbm,
    xs, normed, stat, up_v, down_v, send1, recv1, send2, recv2, out_v,
    x_sem, up_sem, down_sem, out_sem, local_sem, send_sem, recv_sem,
):
    n = sections * experts
    tokens, width = xs.shape
    half = send1.shape[2]
    rest = width - half
    hidden_units = up_v.shape[0]
    chunks = hidden_units // chunk
    section = lax.axis_index("section")
    expert = lax.axis_index("expert")
    me = section * experts + expert

    x_parts = x_sem.shape[0]
    x_rows = tokens // x_parts
    x_copies = [
        pltpu.make_async_copy(
            x_hbm.at[pl.ds(i * x_rows, x_rows)], xs.at[pl.ds(i * x_rows, x_rows)], x_sem.at[i]
        )
        for i in range(x_parts)
    ]
    for copy in x_copies:
        copy.start()

    barrier = pltpu.get_barrier_semaphore()

    def coords(k):
        target = lax.rem(me + k, n)
        return target, lax.div(target, experts), lax.rem(target, experts)

    def greet(k, carry):
        _, s, e = coords(k)
        pl.semaphore_signal(barrier, inc=1, device_id={"section": s, "expert": e}, device_id_type=MESH)
        return carry

    lax.fori_loop(1, n, greet, 0)

    up_copies = []
    down_copies = []
    for c in range(chunks):
        rows = pl.ds(c * chunk, chunk)
        up_copies.append(pltpu.make_async_copy(up_hbm.at[rows], up_v.at[rows], up_sem.at[c]))
        down_copies.append(pltpu.make_async_copy(down_hbm.at[rows], down_v.at[rows], down_sem.at[c]))
    for copy in up_copies + down_copies:
        copy.start()

    columns = slot_ref[...].astype(jnp.float32)
    column_norm = jnp.sqrt(jnp.sum(columns * columns, axis=-1, keepdims=True) + epsilon)
    gain = gain_ref[...].astype(jnp.float32)

    step_rows = 16

    def norm_step(i, carry):
        rows = pl.ds(pl.multiple_of(i * step_rows, step_rows), step_rows)
        values = xs[rows, :].astype(jnp.float32)
        spread = jnp.sum(values * values, axis=-1, keepdims=True) * (1.0 / width)
        result = (values * lax.rsqrt(spread + epsilon) * gain).astype(jnp.bfloat16)
        normed[rows, :] = result
        wide = result.astype(jnp.float32)
        square = jnp.sum(wide * wide, axis=-1, keepdims=True)
        stat[rows, :] = jnp.broadcast_to(square, (step_rows, stat.shape[1]))
        return carry

    per = x_rows // step_rows
    for i, copy in enumerate(x_copies):
        copy.wait()
        lax.fori_loop(i * per, (i + 1) * per, norm_step, 0, unroll=True)

    raw = lax.dot_general(slot_ref[...], normed[...], NT, preferred_element_type=jnp.float32)
    token_norm = jnp.sqrt(jnp.transpose(stat[...])[0:1, :] + epsilon)
    logits = scale_ref[0] * raw / (token_norm * column_norm)
    scores = jnp.exp(logits)
    dispatch = (scores / jnp.sum(scores, axis=1, keepdims=True)).astype(jnp.bfloat16)
    combine = (scores / jnp.sum(scores, axis=0, keepdims=True)).astype(jnp.bfloat16)
    slot_in = jnp.dot(dispatch, normed[...], preferred_element_type=jnp.float32).astype(jnp.bfloat16)
    send1[:, 0, :] = slot_in[:, :half]
    send1[:, 1, :rest] = slot_in[:, half:]

    pl.semaphore_wait(barrier, n - 1)

    own1 = pltpu.make_async_copy(send1.at[expert], recv1.at[me], local_sem.at[0])
    own1.start()

    def dispatch_row(k, carry):
        _, s, e = coords(k)
        pltpu.make_async_remote_copy(
            src_ref=send1.at[e], dst_ref=recv1.at[me], send_sem=send_sem.at[0], recv_sem=recv_sem.at[0],
            device_id={"section": s, "expert": e}, device_id_type=MESH,
        ).start()
        return carry

    lax.fori_loop(1, n, dispatch_row, 0)

    def wait_all(buffer, sem):
        part = buffer.at[pl.ds(0, n - 1)]
        pltpu.make_async_copy(part, part, sem).wait()

    own1.wait()
    wait_all(recv1, recv_sem.at[0])
    left = recv1[:, 0, :]
    right = recv1[:, 1, :rest]
    rows_in = jnp.concatenate([left, right], axis=1)
    total = None
    for c in range(chunks):
        rows = pl.ds(c * chunk, chunk)
        up_copies[c].wait()
        pre = lax.dot_general(rows_in, up_v[rows, :], NT, preferred_element_type=jnp.float32)
        act = jax.nn.gelu(pre).astype(jnp.bfloat16)
        down_copies[c].wait()
        term = jnp.dot(act, down_v[rows, :], preferred_element_type=jnp.float32)
        total = term if total is None else total + term
    partial = total.astype(jnp.bfloat16)
    send2[:, 0, :] = partial[:, :half]
    send2[:, 1, :rest] = partial[:, half:]

    own2 = pltpu.make_async_copy(send2.at[me], recv2.at[me], local_sem.at[1])
    own2.start()

    def return_row(k, carry):
        target, s, e = coords(k)
        pltpu.make_async_remote_copy(
            src_ref=send2.at[target], dst_ref=recv2.at[me], send_sem=send_sem.at[1], recv_sem=recv_sem.at[1],
            device_id={"section": s, "expert": e}, device_id_type=MESH,
        ).start()
        return carry

    lax.fori_loop(1, n, return_row, 0)

    own2.wait()
    wait_all(recv2, recv_sem.at[1])
    summed = recv2[pl.ds(0, experts)].astype(jnp.float32)
    for s in range(1, sections):
        summed = summed + recv2[pl.ds(s * experts, experts)].astype(jnp.float32)
    slot_out = summed.astype(jnp.bfloat16)
    slot_out = jnp.concatenate([slot_out[:, 0, :], slot_out[:, 1, :rest]], axis=1)

    o_parts = out_sem.shape[0]
    o_rows = tokens // o_parts
    copies = []
    for i in range(o_parts):
        rows = pl.ds(i * o_rows, o_rows)
        mixed = lax.dot_general(
            combine[:, i * o_rows:(i + 1) * o_rows], slot_out, TN, preferred_element_type=jnp.float32
        )
        out_v[rows, :] = (xs[rows, :].astype(jnp.float32) + mixed).astype(jnp.bfloat16)
        copy = pltpu.make_async_copy(out_v.at[rows], out_hbm.at[rows], out_sem.at[i])
        copy.start()
        copies.append(copy)
    wait_all(recv1, send_sem.at[0])
    wait_all(recv2, send_sem.at[1])
    for copy in copies:
        copy.wait()


def solution(mesh):
    sections, experts = mesh.shape["section"], mesh.shape["expert"]
    n = sections * experts

    def local(images, norm_gain, slot_map, logit_scale, up_weight, down_weight):
        count, tokens, width = images.shape
        held, hidden_units, _ = up_weight.shape
        slots = slot_map.shape[1]
        assert count == 1 and held == 1 and slots == experts
        half = -(-width // 256) * 128
        chunk = split_of(hidden_units, 512, 128)
        chunks = hidden_units // chunk
        bf16 = jnp.bfloat16
        hbm = pl.BlockSpec(memory_space=pl.ANY)
        vmem = pl.BlockSpec(memory_space=pltpu.VMEM)
        x_parts, o_parts = 4, 2
        result = pl.pallas_call(
            functools.partial(kernel, sections, experts, chunk),
            out_shape=jax.ShapeDtypeStruct((tokens, width), bf16),
            in_specs=[hbm, vmem, vmem, pl.BlockSpec(memory_space=pltpu.SMEM), hbm, hbm],
            out_specs=hbm,
            scratch_shapes=[
                pltpu.VMEM((tokens, width), bf16),
                pltpu.VMEM((tokens, width), bf16),
                pltpu.VMEM((tokens, 128), jnp.float32),
                pltpu.VMEM((hidden_units, width), bf16),
                pltpu.VMEM((hidden_units, width), bf16),
                pltpu.VMEM((experts, 2, half), bf16),
                pltpu.VMEM((n, 2, half), bf16),
                pltpu.VMEM((n, 2, half), bf16),
                pltpu.VMEM((n, 2, half), bf16),
                pltpu.VMEM((tokens, width), bf16),
                pltpu.SemaphoreType.DMA((x_parts,)),
                pltpu.SemaphoreType.DMA((chunks,)),
                pltpu.SemaphoreType.DMA((chunks,)),
                pltpu.SemaphoreType.DMA((o_parts,)),
                pltpu.SemaphoreType.DMA((2,)),
                pltpu.SemaphoreType.DMA((2,)),
                pltpu.SemaphoreType.DMA((2,)),
            ],
            compiler_params=pltpu.CompilerParams(
                collective_id=0, has_side_effects=True, vmem_limit_bytes=60 * 1024 * 1024
            ),
        )(
            images.reshape(tokens, width), norm_gain.reshape(1, width), slot_map.T, logit_scale,
            up_weight.reshape(hidden_units, width), down_weight.reshape(hidden_units, width),
        )
        return result.reshape(1, tokens, width)

    return jax.shard_map(
        local,
        mesh=mesh,
        in_specs=(
            P(("section", "expert"), None, None),
            P(),
            P(),
            P(),
            P("expert", "section", None),
            P("expert", "section", None),
        ),
        out_specs=P(("section", "expert"), None, None),
        check_vma=False,
    )
```

```python
import functools

import jax
import jax.numpy as jnp
from jax import lax
from jax.experimental import pallas as pl
from jax.experimental.pallas import tpu as pltpu
from jax.sharding import PartitionSpec as P

epsilon = 1e-06
MESH = pl.DeviceIdType.MESH
NT = (((1,), (1,)), ((), ()))
TN = (((0,), (0,)), ((), ()))


def split_of(total, most, unit):
    best = unit
    for size in range(unit, most + 1, unit):
        if total % size == 0:
            best = size
    return best


def kernel(
    sections, experts, chunk,
    x_hbm, gain_ref, slot_ref, scale_ref, up_hbm, down_hbm,
    out_v,
    xs, normed, stat, up_v, down_v, send1, recv1, send2, recv2,
    x_sem, up_sem, down_sem, local_sem, send_sem, recv_sem,
):
    n = sections * experts
    tokens, width = xs.shape
    half = send1.shape[2]
    rest = width - half
    hidden_units = up_v.shape[0]
    chunks = hidden_units // chunk
    section = lax.axis_index("section")
    expert = lax.axis_index("expert")
    me = section * experts + expert

    x_parts = x_sem.shape[0]
    x_rows = tokens // x_parts
    x_copies = [
        pltpu.make_async_copy(
            x_hbm.at[pl.ds(i * x_rows, x_rows)], xs.at[pl.ds(i * x_rows, x_rows)], x_sem.at[i]
        )
        for i in range(x_parts)
    ]
    for copy in x_copies:
        copy.start()

    barrier = pltpu.get_barrier_semaphore()

    def wrapped(value, bound):
        return jnp.where(value >= bound, value - bound, value)

    def for_others(visit):
        def step(k, carry):
            s = wrapped(section + k // experts, sections)
            e = wrapped(expert + k % experts, experts)
            visit(s * experts + e, e, {"section": s, "expert": e})
            return carry

        if n <= 64:
            for k in range(n - 1, 0, -1):
                step(k, 0)
        else:
            lax.fori_loop(1, n, step, 0)

    def greet(target, e, device):
        pl.semaphore_signal(barrier, inc=1, device_id=device, device_id_type=MESH)

    for_others(greet)

    up_copies = []
    down_copies = []
    for c in range(chunks):
        rows = pl.ds(c * chunk, chunk)
        up_copies.append(pltpu.make_async_copy(up_hbm.at[rows], up_v.at[rows], up_sem.at[c]))
        down_copies.append(pltpu.make_async_copy(down_hbm.at[rows], down_v.at[rows], down_sem.at[c]))
    for copy in up_copies + down_copies:
        copy.start()

    columns = slot_ref[...].astype(jnp.float32)
    column_norm = jnp.sqrt(jnp.sum(columns * columns, axis=-1, keepdims=True) + epsilon)
    gain = gain_ref[...].astype(jnp.float32).reshape(1, width)

    step_rows = 16

    def norm_step(i, carry):
        rows = pl.ds(pl.multiple_of(i * step_rows, step_rows), step_rows)
        values = xs[rows, :].astype(jnp.float32)
        spread = jnp.sum(values * values, axis=-1, keepdims=True) * (1.0 / width)
        result = (values * lax.rsqrt(spread + epsilon) * gain).astype(jnp.bfloat16)
        normed[rows, :] = result
        wide = result.astype(jnp.float32)
        square = jnp.sum(wide * wide, axis=-1, keepdims=True)
        stat[rows, :] = jnp.broadcast_to(square, (step_rows, stat.shape[1]))
        return carry

    per = x_rows // step_rows
    for i, copy in enumerate(x_copies):
        copy.wait()
        lax.fori_loop(i * per, (i + 1) * per, norm_step, 0, unroll=True)

    raw = lax.dot_general(slot_ref[...], normed[...], NT, preferred_element_type=jnp.float32)
    token_norm = jnp.sqrt(jnp.transpose(stat[...])[0:1, :] + epsilon)
    logits = scale_ref[0] * raw / (token_norm * column_norm)
    scores = jnp.exp(logits)
    dispatch = (scores / jnp.sum(scores, axis=1, keepdims=True)).astype(jnp.bfloat16)
    combine = (scores / jnp.sum(scores, axis=0, keepdims=True)).astype(jnp.bfloat16)
    slot_in = jnp.dot(dispatch, normed[...], preferred_element_type=jnp.float32).astype(jnp.bfloat16)
    send1[:, 0, :] = slot_in[:, :half]
    send1[:, 1, :rest] = slot_in[:, half:]

    pl.semaphore_wait(barrier, n - 1)

    own1 = pltpu.make_async_copy(send1.at[expert], recv1.at[me], local_sem.at[0])
    own1.start()

    def dispatch_row(target, e, device):
        pltpu.make_async_remote_copy(
            src_ref=send1.at[e], dst_ref=recv1.at[me], send_sem=send_sem.at[0], recv_sem=recv_sem.at[0],
            device_id=device, device_id_type=MESH,
        ).start()

    for_others(dispatch_row)

    def wait_all(buffer, sem):
        part = buffer.at[pl.ds(0, n - 1)]
        pltpu.make_async_copy(part, part, sem).wait()

    own1.wait()
    wait_all(recv1, recv_sem.at[0])
    left = recv1[:, 0, :]
    right = recv1[:, 1, :rest]
    rows_in = jnp.concatenate([left, right], axis=1)
    total = None
    for c in range(chunks):
        rows = pl.ds(c * chunk, chunk)
        up_copies[c].wait()
        pre = lax.dot_general(rows_in, up_v[rows, :], NT, preferred_element_type=jnp.float32)
        act = jax.nn.gelu(pre).astype(jnp.bfloat16)
        down_copies[c].wait()
        term = jnp.dot(act, down_v[rows, :], preferred_element_type=jnp.float32)
        total = term if total is None else total + term
    partial = total.astype(jnp.bfloat16)
    send2[:, 0, :] = partial[:, :half]
    send2[:, 1, :rest] = partial[:, half:]

    own2 = pltpu.make_async_copy(send2.at[me], recv2.at[me], local_sem.at[1])
    own2.start()

    def return_row(target, e, device):
        pltpu.make_async_remote_copy(
            src_ref=send2.at[target], dst_ref=recv2.at[me], send_sem=send_sem.at[1], recv_sem=recv_sem.at[1],
            device_id=device, device_id_type=MESH,
        ).start()

    for_others(return_row)

    own2.wait()
    wait_all(recv2, recv_sem.at[1])
    summed = recv2[pl.ds(0, experts)].astype(jnp.float32)
    for s in range(1, sections):
        summed = summed + recv2[pl.ds(s * experts, experts)].astype(jnp.float32)
    slot_out = summed.astype(jnp.bfloat16)
    slot_out = jnp.concatenate([slot_out[:, 0, :], slot_out[:, 1, :rest]], axis=1)

    o_parts = 4
    o_rows = tokens // o_parts
    for i in range(o_parts):
        rows = pl.ds(i * o_rows, o_rows)
        mixed = lax.dot_general(
            combine[:, i * o_rows:(i + 1) * o_rows], slot_out, TN, preferred_element_type=jnp.float32
        )
        out_v[rows, :] = (xs[rows, :].astype(jnp.float32) + mixed).astype(jnp.bfloat16)
    wait_all(recv1, send_sem.at[0])
    wait_all(recv2, send_sem.at[1])


def solution(mesh):
    sections, experts = mesh.shape["section"], mesh.shape["expert"]
    n = sections * experts

    def local(images, norm_gain, slot_map, logit_scale, up_weight, down_weight):
        count, tokens, width = images.shape
        held, hidden_units, _ = up_weight.shape
        slots = slot_map.shape[1]
        assert count == 1 and held == 1 and slots == experts
        half = -(-width // 256) * 128
        chunk = split_of(hidden_units, 512, 128)
        chunks = hidden_units // chunk
        bf16 = jnp.bfloat16
        hbm = pl.BlockSpec(memory_space=pl.ANY)
        vmem = pl.BlockSpec(memory_space=pltpu.VMEM)
        x_parts = 4
        result = pl.pallas_call(
            functools.partial(kernel, sections, experts, chunk),
            out_shape=pltpu.VMEM((tokens, width), bf16),
            in_specs=[hbm, vmem, vmem, pl.BlockSpec(memory_space=pltpu.SMEM), hbm, hbm],
            out_specs=vmem,
            scratch_shapes=[
                pltpu.VMEM((tokens, width), bf16),
                pltpu.VMEM((tokens, width), bf16),
                pltpu.VMEM((tokens, 128), jnp.float32),
                pltpu.VMEM((hidden_units, width), bf16),
                pltpu.VMEM((hidden_units, width), bf16),
                pltpu.VMEM((experts, 2, half), bf16),
                pltpu.VMEM((n, 2, half), bf16),
                pltpu.VMEM((n, 2, half), bf16),
                pltpu.VMEM((n, 2, half), bf16),
                pltpu.SemaphoreType.DMA((x_parts,)),
                pltpu.SemaphoreType.DMA((chunks,)),
                pltpu.SemaphoreType.DMA((chunks,)),
                pltpu.SemaphoreType.DMA((2,)),
                pltpu.SemaphoreType.DMA((2,)),
                pltpu.SemaphoreType.DMA((2,)),
            ],
            compiler_params=pltpu.CompilerParams(
                collective_id=0, has_side_effects=True, vmem_limit_bytes=60 * 1024 * 1024
            ),
        )(
            images.reshape(tokens, width), norm_gain, slot_map.T, logit_scale,
            up_weight.reshape(hidden_units, width), down_weight.reshape(hidden_units, width),
        )
        return result.reshape(1, tokens, width)

    return jax.shard_map(
        local,
        mesh=mesh,
        in_specs=(
            P(("section", "expert"), None, None),
            P(),
            P(),
            P(),
            P("expert", "section", None),
            P("expert", "section", None),
        ),
        out_specs=P(("section", "expert"), None, None),
        check_vma=False,
    )
```

```python
import functools

import jax
import jax.numpy as jnp
from jax import lax
from jax.experimental import pallas as pl
from jax.experimental.pallas import tpu as pltpu
from jax.sharding import PartitionSpec as P

epsilon = 1e-06
MESH = pl.DeviceIdType.MESH
NT = (((1,), (1,)), ((), ()))
TN = (((0,), (0,)), ((), ()))


def split_of(total, most, unit):
    best = unit
    for size in range(unit, most + 1, unit):
        if total % size == 0:
            best = size
    return best


def kernel(
    sections, experts, chunk,
    x_hbm, gain_ref, slot_ref, scale_ref, up_hbm, down_hbm,
    out_v,
    xs, normed, stat, up_v, down_v, send1, recv1, send2, recv2,
    x_sem, up_sem, down_sem, local_sem, send_sem, recv_sem,
):
    n = sections * experts
    tokens, width = xs.shape
    half = send1.shape[2]
    rest = width - half
    hidden_units = up_v.shape[0]
    chunks = hidden_units // chunk
    section = lax.axis_index("section")
    expert = lax.axis_index("expert")
    me = section * experts + expert

    x_parts = x_sem.shape[0]
    x_rows = tokens // x_parts
    x_copies = [
        pltpu.make_async_copy(
            x_hbm.at[pl.ds(i * x_rows, x_rows)], xs.at[pl.ds(i * x_rows, x_rows)], x_sem.at[i]
        )
        for i in range(x_parts)
    ]
    for copy in x_copies:
        copy.start()

    barrier = pltpu.get_barrier_semaphore()

    def wrapped(value, bound):
        return jnp.where(value >= bound, value - bound, value)

    def for_others(visit):
        def step(k, carry):
            s = wrapped(section + k // experts, sections)
            e = wrapped(expert + k % experts, experts)
            visit(s * experts + e, e, {"section": s, "expert": e})
            return carry

        if n <= 64:
            for k in range(n - 1, 0, -1):
                step(k, 0)
        else:
            lax.fori_loop(1, n, step, 0)

    def greet(target, e, device):
        pl.semaphore_signal(barrier, inc=1, device_id=device, device_id_type=MESH)

    for_others(greet)

    up_copies = []
    down_copies = []
    for c in range(chunks):
        rows = pl.ds(c * chunk, chunk)
        up_copies.append(pltpu.make_async_copy(up_hbm.at[rows], up_v.at[rows], up_sem.at[c]))
        down_copies.append(pltpu.make_async_copy(down_hbm.at[rows], down_v.at[rows], down_sem.at[c]))
    for copy in up_copies + down_copies:
        copy.start()

    columns = slot_ref[...].astype(jnp.float32)
    column_norm = jnp.sqrt(jnp.sum(columns * columns, axis=-1, keepdims=True) + epsilon)
    gain = gain_ref[...].astype(jnp.float32).reshape(1, width)

    step_rows = 16

    def norm_step(i, carry):
        rows = pl.ds(pl.multiple_of(i * step_rows, step_rows), step_rows)
        values = xs[rows, :].astype(jnp.float32)
        spread = jnp.sum(values * values, axis=-1, keepdims=True) * (1.0 / width)
        result = (values * lax.rsqrt(spread + epsilon) * gain).astype(jnp.bfloat16)
        normed[rows, :] = result
        wide = result.astype(jnp.float32)
        square = jnp.sum(wide * wide, axis=-1, keepdims=True)
        stat[rows, :] = jnp.broadcast_to(square, (step_rows, stat.shape[1]))
        return carry

    per = x_rows // step_rows
    for i, copy in enumerate(x_copies):
        copy.wait()
        lax.fori_loop(i * per, (i + 1) * per, norm_step, 0, unroll=True)

    raw = lax.dot_general(slot_ref[...], normed[...], NT, preferred_element_type=jnp.float32)
    token_norm = jnp.sqrt(jnp.transpose(stat[...])[0:1, :] + epsilon)
    logits = scale_ref[0] * raw / (token_norm * column_norm)
    scores = jnp.exp(logits)
    dispatch = (scores / jnp.sum(scores, axis=1, keepdims=True)).astype(jnp.bfloat16)
    combine = (scores / jnp.sum(scores, axis=0, keepdims=True)).astype(jnp.bfloat16)
    slot_in = jnp.dot(dispatch, normed[...], preferred_element_type=jnp.float32).astype(jnp.bfloat16)
    send1[:, 0, :] = slot_in[:, :half]
    send1[:, 1, :rest] = slot_in[:, half:]

    pl.semaphore_wait(barrier, n - 1)

    own1 = pltpu.make_async_copy(send1.at[expert], recv1.at[me], local_sem.at[0])
    own1.start()

    def dispatch_row(target, e, device):
        pltpu.make_async_remote_copy(
            src_ref=send1.at[e], dst_ref=recv1.at[me], send_sem=send_sem.at[0], recv_sem=recv_sem.at[0],
            device_id=device, device_id_type=MESH,
        ).start()

    for_others(dispatch_row)

    def wait_all(buffer, sem):
        part = buffer.at[pl.ds(0, n - 1)]
        pltpu.make_async_copy(part, part, sem).wait()

    own1.wait()
    wait_all(recv1, recv_sem.at[0])
    left = recv1[:, 0, :]
    right = recv1[:, 1, :rest]
    rows_in = jnp.concatenate([left, right], axis=1)
    total = None
    for c in range(chunks):
        rows = pl.ds(c * chunk, chunk)
        up_copies[c].wait()
        pre = lax.dot_general(rows_in, up_v[rows, :], NT, preferred_element_type=jnp.float32)
        act = jax.nn.gelu(pre).astype(jnp.bfloat16)
        down_copies[c].wait()
        term = jnp.dot(act, down_v[rows, :], preferred_element_type=jnp.float32)
        total = term if total is None else total + term
    partial = total.astype(jnp.bfloat16)
    send2[:, 0, :] = partial[:, :half]
    send2[:, 1, :rest] = partial[:, half:]

    own2 = pltpu.make_async_copy(send2.at[me], recv2.at[me], local_sem.at[1])
    own2.start()

    def return_row(target, e, device):
        pltpu.make_async_remote_copy(
            src_ref=send2.at[target], dst_ref=recv2.at[me], send_sem=send_sem.at[1], recv_sem=recv_sem.at[1],
            device_id=device, device_id_type=MESH,
        ).start()

    for_others(return_row)

    own2.wait()
    wait_all(recv2, recv_sem.at[1])
    summed = recv2[pl.ds(0, experts)].astype(jnp.float32)
    for s in range(1, sections):
        summed = summed + recv2[pl.ds(s * experts, experts)].astype(jnp.float32)
    slot_out = summed.astype(jnp.bfloat16)
    slot_out = jnp.concatenate([slot_out[:, 0, :], slot_out[:, 1, :rest]], axis=1)

    o_parts = 4
    o_rows = tokens // o_parts
    for i in range(o_parts):
        rows = pl.ds(i * o_rows, o_rows)
        mixed = lax.dot_general(
            combine[:, i * o_rows:(i + 1) * o_rows], slot_out, TN, preferred_element_type=jnp.float32
        )
        out_v[rows, :] = (xs[rows, :].astype(jnp.float32) + mixed).astype(jnp.bfloat16)
    wait_all(recv1, send_sem.at[0])
    wait_all(recv2, send_sem.at[1])


def solution(mesh):
    sections, experts = mesh.shape["section"], mesh.shape["expert"]
    n = sections * experts

    def local(images, norm_gain, slot_map, logit_scale, up_weight, down_weight):
        count, tokens, width = images.shape
        held, hidden_units, _ = up_weight.shape
        slots = slot_map.shape[1]
        assert count == 1 and held == 1 and slots == experts
        half = -(-width // 256) * 128
        chunk = split_of(hidden_units, 1280, 128)
        chunks = hidden_units // chunk
        bf16 = jnp.bfloat16
        hbm = pl.BlockSpec(memory_space=pl.ANY)
        vmem = pl.BlockSpec(memory_space=pltpu.VMEM)
        x_parts = 4
        result = pl.pallas_call(
            functools.partial(kernel, sections, experts, chunk),
            out_shape=pltpu.VMEM((tokens, width), bf16),
            in_specs=[hbm, vmem, vmem, pl.BlockSpec(memory_space=pltpu.SMEM), hbm, hbm],
            out_specs=vmem,
            scratch_shapes=[
                pltpu.VMEM((tokens, width), bf16),
                pltpu.VMEM((tokens, width), bf16),
                pltpu.VMEM((tokens, 128), jnp.float32),
                pltpu.VMEM((hidden_units, width), bf16),
                pltpu.VMEM((hidden_units, width), bf16),
                pltpu.VMEM((experts, 2, half), bf16),
                pltpu.VMEM((n, 2, half), bf16),
                pltpu.VMEM((n, 2, half), bf16),
                pltpu.VMEM((n, 2, half), bf16),
                pltpu.SemaphoreType.DMA((x_parts,)),
                pltpu.SemaphoreType.DMA((chunks,)),
                pltpu.SemaphoreType.DMA((chunks,)),
                pltpu.SemaphoreType.DMA((2,)),
                pltpu.SemaphoreType.DMA((2,)),
                pltpu.SemaphoreType.DMA((2,)),
            ],
            compiler_params=pltpu.CompilerParams(
                collective_id=0, has_side_effects=True, vmem_limit_bytes=60 * 1024 * 1024
            ),
        )(
            images.reshape(tokens, width), norm_gain, slot_map.T, logit_scale,
            up_weight.reshape(hidden_units, width), down_weight.reshape(hidden_units, width),
        )
        return result.reshape(1, tokens, width)

    return jax.shard_map(
        local,
        mesh=mesh,
        in_specs=(
            P(("section", "expert"), None, None),
            P(),
            P(),
            P(),
            P("expert", "section", None),
            P("expert", "section", None),
        ),
        out_specs=P(("section", "expert"), None, None),
        check_vma=False,
    )
```
